32 devices in a mesh: seq: 16 (over z, x, core), head: 2 (over y).
Axes of the slice: x: 2, y: 2, z: 4, core: 2. Of those that a mesh axis runs over, the one named last changes fastest.
Arguments:
- tokens: bfloat16 [8192, 1024], P('seq'), may hold values from -6 to 6
- mem_query_w: bfloat16 [1024, 1024], P(None, 'head'), may hold values from -0.1875 to 0.1875
- mem_key_w: bfloat16 [1024, 1024], P(None, 'head'), may hold values from -0.1875 to 0.1875
- mem_value_w: bfloat16 [1024, 1024], P(None, 'head'), may hold values from -0.1875 to 0.1875
- mem_in: float32 [1024, 1024], P(None, 'head'), may hold values from -0.1875 to 0.1875
- mem_out: float32 [1024, 1024], P('head'), may hold values from -0.1875 to 0.1875
- forget_levels: float32 [16, 1024], P(None, 'head'), may hold values from 0.003 to 0.3
- momentum_levels: float32 [16, 1024], P(None, 'head'), may hold values from 0.2 to 0.9
- step_levels: float32 [16, 1024], P(None, 'head'), may hold values from 0.02 to 0.2
- plan: int32 [16], P('seq'), may hold values from 0 to 15
- norm_gain: float32 [1024], replicated, may hold values from 0.5 to 1.5
- attn_query_w: bfloat16 [1024, 1024], P(None, 'head'), may hold values from -1 to 1
- attn_key_w: bfloat16 [1024, 1024], P(None, 'head'), may hold values from -4 to 4
- attn_value_w: bfloat16 [1024, 1024], P(None, 'head'), may hold values from -0.1875 to 0.1875
- attn_out_w: bfloat16 [1024, 1024], P('head'), may hold values from -0.25 to 0.25
Outputs:
- layer_out: bfloat16 [8192, 1024], P('seq', 'head')
The draws below stay inside these ranges and needn't reach their ends.
All inputs are finite; a program needn't handle non-finite values.
Results may differ from the reference program's by a relative error of at most 0.014.
Values may be sent and summed in bfloat16 or wider, within the bound.
A program may use at most 192 MiB of HBM per device.

```python
import math
import jax
import jax.numpy as jnp
from jax import lax

D = 1024
HEAD_DIM = 64
MEM_HID = 1024
LEVELS = 16
SPAN = 8
TOK_DEV = 512
GROUPS = 16
LENGTH = 8192


def attention_pair(key):
    shared = jax.random.normal(jax.random.fold_in(key, 11), (D, D), jnp.float32) / math.sqrt(D)
    others = jax.random.normal(jax.random.fold_in(key, 12), (D, D), jnp.float32) / math.sqrt(D)
    return (shared, others)


def draw_attn_query_w(key, part):
    shared, others = attention_pair(key)
    return jnp.clip(shared, -1.0, 1.0).astype(jnp.bfloat16)


def draw_attn_key_w(key, part):
    shared, others = attention_pair(key)
    return jnp.clip(others, -4.0, 4.0).astype(jnp.bfloat16)


def touch_ends(array, key, smallest, largest):
    extent = array.shape
    spot = [jax.random.randint(jax.random.fold_in(key, axis), (), 0, extent[axis]) for axis in range(len(extent))]
    array = array.at[tuple(spot)].set(smallest)
    longest = extent.index(max(extent))
    spot[longest] = (spot[longest] + 1) % extent[longest]
    return array.at[tuple(spot)].set(largest)


def spiked(drawn, stream_key, source, target, shards_of, factor):
    def block_of(position):
        return (jnp.arange(drawn.shape[position]) // (drawn.shape[position] // shards_of)).reshape((-1,) + (1,) * (drawn.ndim - 1 - position))

    near = jax.random.permutation(stream_key, shards_of)[block_of(target)]
    far = (block_of(target) + shards_of // 2) % shards_of
    return jnp.where((block_of(source) == near) | (block_of(source) == far), factor * drawn, drawn)


def shard_levels(own_key, extent, split, least, largest):
    factor_of = 1.0
    for position, shards_of in split:
        steps = jax.random.uniform(jax.random.fold_in(jax.random.fold_in(own_key, 6), position), (shards_of,), jnp.float32, least / len(split), largest / len(split))
        factor_of = factor_of * jnp.repeat(jnp.exp(steps), extent[position] // shards_of).reshape((-1,) + (1,) * (len(extent) - 1 - position))
    return factor_of


def scatter_about(rng, extent, spread, most, split=(), kind=jnp.bfloat16):
    factor_of = shard_levels(rng, extent, split, -0.22, 0.18) if split else 1.0
    result = jax.random.normal(rng, extent, jnp.float32) * spread * factor_of
    return jnp.minimum(jnp.maximum(result, -most), most).astype(kind)


def heavy_noise(own_key, dims, width, limit, shards, heavy, kind=jnp.bfloat16):
    result = width * jax.random.normal(own_key, dims, jnp.float32)
    if shards:
        result = result * shard_levels(own_key, dims, shards, -0.22, 0.18)
    return jnp.clip(spiked(result, jax.random.fold_in(own_key, 3), *heavy), -limit, limit).astype(kind)


def setup_inputs(seed: int = 0) -> dict:
    splits = jax.random.split(jax.random.key(seed), 16)
    tokens = scatter_about(splits[0], (LENGTH, D), 1.0, 6.0, ((0, 16),))
    mem_query_w = scatter_about(splits[1], (D, D), D ** -0.5, 0.1875, ((1, 2),))
    mem_key_w = scatter_about(splits[2], (D, D), D ** -0.5, 0.1875, ((1, 2),))
    mem_value_w = scatter_about(splits[3], (D, D), D ** -0.5, 0.1875, ((1, 2),))
    mem_in = scatter_about(splits[4], (D, MEM_HID), D ** -0.5, 0.1875, ((1, 2),), jnp.float32)
    mem_out = scatter_about(splits[5], (MEM_HID, D), MEM_HID ** -0.5, 0.1875, ((0, 2),), jnp.float32)
    forget_levels = jnp.clip(jnp.exp(math.log(0.3) - 4.6051702 * jax.random.uniform(splits[6], (LEVELS, MEM_HID), jnp.float32) ** shard_levels(splits[6], (LEVELS, MEM_HID), ((1, 2),), -0.2, 0.2)), 0.003, 0.3)
    momentum_levels = jnp.clip(0.2 + 0.7 * jax.random.uniform(splits[7], (LEVELS, MEM_HID), jnp.float32) ** shard_levels(splits[7], (LEVELS, MEM_HID), ((1, 2),), -0.2, 0.2), 0.2, 0.9)
    step_levels = jnp.clip(jnp.exp(math.log(0.2) - 2.3025851 * jax.random.uniform(splits[8], (LEVELS, MEM_HID), jnp.float32) ** shard_levels(splits[8], (LEVELS, MEM_HID), ((1, 2),), -0.2, 0.2)), 0.02, 0.2)
    plan = touch_ends(jax.random.randint(splits[9], (GROUPS,), 0, LEVELS), jax.random.fold_in(splits[9], 1), 0, LEVELS - 1).astype(jnp.int32)
    norm_gain = jnp.clip(1.0 + 0.1 * jax.random.normal(splits[10], (D,), jnp.float32), 0.5, 1.5)
    attn_query_w = draw_attn_query_w(jax.random.fold_in(splits[15], 71), 0)
    attn_key_w = draw_attn_key_w(jax.random.fold_in(splits[15], 71), 0)
    attn_value_w = scatter_about(splits[13], (D, D), D ** -0.5, 0.1875, ((1, 2),))
    attn_out_w = heavy_noise(splits[14], (D, D), D ** -0.5, 0.25, ((0, 2),), (0, 1, 2, 2.0))
    return {"tokens": tokens, "mem_query_w": mem_query_w, "mem_key_w": mem_key_w, "mem_value_w": mem_value_w, "mem_in": mem_in, "mem_out": mem_out, "forget_levels": forget_levels, "momentum_levels": momentum_levels, "step_levels": step_levels, "plan": plan, "norm_gain": norm_gain, "attn_query_w": attn_query_w, "attn_key_w": attn_key_w, "attn_value_w": attn_value_w, "attn_out_w": attn_out_w}


highest = lax.Precision.HIGHEST
epsilon = 1e-06

def silu_slope(values):
    sigmoid = jax.nn.sigmoid(values)
    return sigmoid * (1.0 + values * (1.0 - sigmoid))

def project(left, weight):
    return jnp.dot(left, weight, preferred_element_type=jnp.float32).astype(jnp.bfloat16)

def normalize(retrieved, norm_gain):
    mean_square = lax.optimization_barrier(jnp.mean(retrieved * retrieved, axis=-1, keepdims=True))
    return (retrieved * lax.rsqrt(mean_square + epsilon) * norm_gain).astype(jnp.bfloat16)

def window_attend(query, keys, values, block_index, head_dim):
    query_count = query.shape[0]
    key_count = keys.shape[0]
    head_count = query.shape[1] // head_dim
    query_heads = query.reshape(query_count, head_count, head_dim).astype(jnp.float32)
    key_heads = keys.reshape(key_count, head_count, head_dim).astype(jnp.float32)
    value_heads = values.reshape(key_count, head_count, head_dim).astype(jnp.float32)
    scores = jnp.einsum('qhd,khd->hqk', query_heads, key_heads) * head_dim ** (-0.5)
    span_rows = key_count - query_count
    distance = span_rows + jnp.arange(query_count, dtype=jnp.int32)[:, None] - jnp.arange(key_count, dtype=jnp.int32)[None, :]
    key_pos = (block_index * query_count - span_rows + jnp.arange(key_count, dtype=jnp.int32))[None, :]
    allowed = (distance >= 0) & (distance < span_rows) & (key_pos >= 0)
    scores = jnp.where(allowed[None], scores, -1e+30)
    row_peak = lax.optimization_barrier(jnp.max(scores, axis=-1, keepdims=True))
    weights = jnp.exp(scores - row_peak)
    probabilities = (weights / lax.optimization_barrier(jnp.sum(weights, axis=-1, keepdims=True))).astype(jnp.bfloat16)
    context = jnp.einsum('hqk,khd->qhd', probabilities.astype(jnp.float32), value_heads)
    return context.reshape(query_count, head_count * head_dim).astype(jnp.bfloat16)

def reference(tokens, mem_query_w, mem_key_w, mem_value_w, mem_in, mem_out, forget_levels, momentum_levels, step_levels, plan, norm_gain, attn_query_w, attn_key_w, attn_value_w, attn_out_w):
    mem_query = project(tokens, mem_query_w).reshape(GROUPS, TOK_DEV, D)
    mem_key = project(tokens, mem_key_w).reshape(GROUPS, TOK_DEV, D)
    mem_value = project(tokens, mem_value_w).reshape(GROUPS, TOK_DEV, D)

    def group_step(state_now, inputs):
        speed_in, speed_out, weight_in, weight_out = state_now
        query_rows, key_rows, value_rows, chosen = inputs
        keys_wide = key_rows.astype(jnp.float32)
        pre_act = jnp.dot(keys_wide, mem_in, precision=highest)
        hidden = jax.nn.silu(pre_act)
        predicted = jnp.dot(hidden, mem_out, precision=highest)
        residual_err = 2.0 / TOK_DEV * (predicted - value_rows.astype(jnp.float32))
        grad_out = jnp.dot(hidden.T, residual_err, precision=highest)
        slope_term = jnp.dot(residual_err, mem_out.T, precision=highest) * silu_slope(pre_act)
        grad_in = jnp.dot(keys_wide.T, slope_term, precision=highest)
        query_wide = query_rows.astype(jnp.float32)
        retrieved = jnp.dot(jax.nn.silu(jnp.dot(query_wide, weight_in, precision=highest)), weight_out, precision=highest)
        forget = forget_levels[chosen]
        momentum = momentum_levels[chosen]
        step_rate = step_levels[chosen]
        speed_in = momentum[None, :] * speed_in - step_rate[None, :] * grad_in
        speed_out = momentum[:, None] * speed_out - step_rate[:, None] * grad_out
        weight_in = (1.0 - forget)[None, :] * weight_in + speed_in
        weight_out = (1.0 - forget)[:, None] * weight_out + speed_out
        return ((speed_in, speed_out, weight_in, weight_out), retrieved)
    initial = (jnp.zeros_like(mem_in), jnp.zeros_like(mem_out), mem_in, mem_out)
    last_state, retrieved = lax.scan(group_step, initial, (mem_query, mem_key, mem_value, plan))
    normed = normalize(retrieved.reshape(LENGTH, D), norm_gain)
    att_query = project(normed, attn_query_w)
    att_key = project(normed, attn_key_w)
    att_value = project(normed, attn_value_w)
    span_rows = SPAN * TOK_DEV
    padding = jnp.zeros((span_rows, D), jnp.bfloat16)
    key_padded = jnp.concatenate([padding, att_key], axis=0)
    value_padded = jnp.concatenate([padding, att_value], axis=0)

    def attend_block(block_index):
        begin = block_index * TOK_DEV
        query_block = lax.dynamic_slice_in_dim(att_query, begin, TOK_DEV, 0)
        key_block = lax.dynamic_slice_in_dim(key_padded, begin, span_rows + TOK_DEV, 0)
        value_block = lax.dynamic_slice_in_dim(value_padded, begin, span_rows + TOK_DEV, 0)
        return window_attend(query_block, key_block, value_block, block_index, HEAD_DIM)
    context = lax.map(attend_block, jnp.arange(GROUPS, dtype=jnp.int32)).reshape(LENGTH, D)
    return project(context, attn_out_w)
```

```python
import functools
import math

import jax
import jax.numpy as jnp
from jax import lax
from jax.experimental import pallas as pl
from jax.experimental.pallas import tpu as pltpu
from jax.sharding import PartitionSpec as P

HEAD_DIM = 64
LANES = 2 * HEAD_DIM
SPAN = 8
MESH = pl.DeviceIdType.MESH

epsilon = 1e-06
ANY = pl.BlockSpec(memory_space=pl.ANY)
VMEM = pl.BlockSpec(memory_space=pltpu.VMEM)


def meet(axis, n):
    me = lax.axis_index(axis)
    barrier = pltpu.get_barrier_semaphore()
    for k in range(1, n):
        pl.semaphore_signal(
            barrier, inc=1, device_id={axis: lax.rem(me + k, n)}, device_id_type=MESH
        )
    pl.semaphore_wait(barrier, n - 1)


def remote(src, dst, send, recv, axis, peer):
    return pltpu.make_async_remote_copy(
        src_ref=src,
        dst_ref=dst,
        send_sem=send,
        recv_sem=recv,
        device_id={axis: peer},
        device_id_type=MESH,
    )


def part(ref, dim, index, size):
    window = pl.ds(pl.multiple_of(index * size, size), size)
    return ref.at[:, window] if dim == 1 else ref.at[window, :]


def gather_kernel(axis, n, dim, size, x_ref, o_ref, send, recv, local):
    me = lax.axis_index(axis)
    meet(axis, n)
    slot = part(o_ref, dim, me, size)
    copies = []
    for k in range(1, n):
        copy = remote(x_ref, slot, send.at[k - 1], recv.at[k - 1], axis, lax.rem(me + k, n))
        copy.start()
        copies.append(copy)
    own = pltpu.make_async_copy(x_ref, slot, local)
    own.start()
    own.wait()
    for copy in copies:
        copy.wait()


def split_kernel(axis, n, dim, size, x_ref, o_ref, send, recv, local):
    me = lax.axis_index(axis)
    meet(axis, n)
    copies = []
    for k in range(1, n):
        peer = lax.rem(me + k, n)
        copy = remote(
            part(x_ref, dim, peer, size),
            o_ref.at[me],
            send.at[k - 1],
            recv.at[k - 1],
            axis,
            peer,
        )
        copy.start()
        copies.append(copy)
    own = pltpu.make_async_copy(part(x_ref, dim, me, size), o_ref.at[me], local)
    own.start()
    own.wait()
    for copy in copies:
        copy.wait()


def comm_call(kernel, out, n, identity, x):
    return pl.pallas_call(
        kernel,
        out_shape=out,
        in_specs=[ANY],
        out_specs=ANY,
        scratch_shapes=[
            pltpu.SemaphoreType.DMA((n - 1,)),
            pltpu.SemaphoreType.DMA((n - 1,)),
            pltpu.SemaphoreType.DMA,
        ],
        compiler_params=pltpu.CompilerParams(collective_id=identity, has_side_effects=True),
    )(x)


def gather(x, axis, dim, identity):
    n = lax.axis_size(axis)
    shape = list(x.shape)
    shape[dim] *= n
    kernel = functools.partial(gather_kernel, axis, n, dim, x.shape[dim])
    return comm_call(kernel, jax.ShapeDtypeStruct(tuple(shape), x.dtype), n, identity, x)


def scatter_sum(x, axis, dim, identity):
    n = lax.axis_size(axis)
    shape = list(x.shape)
    shape[dim] //= n
    kernel = functools.partial(split_kernel, axis, n, dim, shape[dim])
    parts = comm_call(kernel, jax.ShapeDtypeStruct((n, *shape), x.dtype), n, identity, x)
    return jnp.sum(parts.astype(jnp.float32), axis=0)


def whole_sum(x, axis, identity):
    parts = gather(x, axis, 0, identity).reshape(-1, *x.shape)
    return jnp.sum(parts.astype(jnp.float32), axis=0)


def memory_kernel(
    n, grads_ref, gates_ref, first_ref, o_ref,
    came, gates, wide, stage, send, recv, send_gate, recv_gate, send_back, recv_back, local,
):
    me = lax.axis_index("seq")
    meet("seq", n)
    copies = []
    for k in range(1, n):
        peer = lax.rem(me + k, n)
        gate_copy = remote(
            gates_ref.at[peer], gates.at[me], send_gate.at[k - 1], recv_gate.at[k - 1], "seq", peer
        )
        gate_copy.start()
        copy = remote(
            grads_ref.at[peer], came.at[me], send.at[k - 1], recv.at[k - 1], "seq", peer
        )
        copy.start()
        copies += [gate_copy, copy]
    own_gates = pltpu.make_async_copy(gates_ref.at[me], gates.at[me], local.at[0])
    own_gates.start()
    own = pltpu.make_async_copy(grads_ref.at[me], came.at[me], local.at[1])
    own.start()
    own_gates.wait()
    own.wait()
    for copy in copies:
        copy.wait()

    for g in range(n):
        row = gates[g]
        for which in range(3):
            wide[which, g] = jnp.broadcast_to(row[:, which : which + 1], row.shape)

    def columns(c, carry):
        window = pl.ds(pl.multiple_of(c * 128, 128), 128)
        weight = first_ref[:, window]
        speed = jnp.zeros_like(weight)
        for g in range(n):
            stage[g, :, window] = weight.astype(jnp.bfloat16)
            if g < n - 1:
                grad = came[g, :, window].astype(jnp.float32)
                speed = wide[0, g] * speed - wide[2, g] * grad
                weight = (1.0 - wide[1, g]) * weight + speed
        return carry

    lax.fori_loop(0, first_ref.shape[1] // 128, columns, 0)

    copies = []
    for k in range(1, n):
        peer = lax.rem(me + k, n)
        copy = remote(
            stage.at[peer], o_ref.at[me], send_back.at[k - 1], recv_back.at[k - 1], "seq", peer
        )
        copy.start()
        copies.append(copy)
    own = pltpu.make_async_copy(stage.at[me], o_ref.at[me], local.at[2])
    own.start()
    own.wait()
    for copy in copies:
        copy.wait()


def evolve(grads, gates, first, identity):
    n = grads.shape[0]
    return pl.pallas_call(
        functools.partial(memory_kernel, n),
        out_shape=jax.ShapeDtypeStruct(grads.shape, jnp.bfloat16),
        in_specs=[ANY, ANY, VMEM],
        out_specs=ANY,
        scratch_shapes=[
            pltpu.VMEM(grads.shape, jnp.bfloat16),
            pltpu.VMEM(gates.shape, jnp.float32),
            pltpu.VMEM((3, *gates.shape), jnp.float32),
            pltpu.VMEM(grads.shape, jnp.bfloat16),
            *[pltpu.SemaphoreType.DMA((n - 1,))] * 6,
            pltpu.SemaphoreType.DMA((3,)),
        ],
        compiler_params=pltpu.CompilerParams(collective_id=identity, has_side_effects=True),
    )(grads, gates, first)


def attention_kernel(
    n, heads, q_ref, kv_ref, o_ref,
    q_all, kv_all, ctx, peaks, totals, q_send, q_recv, kv_send, kv_recv, ctx_send, ctx_recv, local,
):
    me = lax.axis_index("seq")
    chunk = me // heads
    head = lax.rem(me, heads)
    other = lax.rem(me + 1, n)
    rows = q_ref.shape[0]
    slots = SPAN + heads
    first_block = chunk * heads - SPAN
    my_slot = me - first_block
    my_tile = lax.rem(me, heads)

    def lanes(ref, which):
        return ref.at[:, pl.ds(pl.multiple_of(which * LANES, LANES), LANES)]

    def outgoing(k):
        peer = lax.rem(me + k, n)
        peer_chunk = peer // heads
        peer_head = lax.rem(peer, heads)
        slot = me - peer_chunk * heads + SPAN
        wanted = jnp.logical_and(slot >= 0, slot < slots)
        same = peer_chunk == chunk
        safe = jnp.where(wanted, slot, 0)
        kv_copy = remote(
            lanes(kv_ref, peer_head), kv_all.at[safe], kv_send.at[k - 1], kv_recv.at[safe], "seq", peer
        )
        q_copy = remote(
            lanes(q_ref, peer_head), q_all.at[my_tile], q_send.at[k - 1], q_recv.at[my_tile], "seq", peer
        )
        return wanted, same, kv_copy, q_copy

    meet("seq", n)
    own_kv = pltpu.make_async_copy(lanes(kv_ref, head), kv_all.at[my_slot], local.at[0])
    own_q = pltpu.make_async_copy(lanes(q_ref, head), q_all.at[my_tile], local.at[1])
    own_kv.start()
    own_q.start()
    for k in range(1, n):
        wanted, same, kv_copy, q_copy = outgoing(k)

        @pl.when(same)
        def _():
            q_copy.start()

        @pl.when(wanted)
        def _():
            kv_copy.start()

    own_kv.wait()
    own_q.wait()

    def await_kv(slot):
        block = first_block + slot

        @pl.when(jnp.logical_and(block >= 0, block != me))
        def _():
            remote(
                kv_all.at[slot], kv_all.at[slot], kv_send.at[0], kv_recv.at[slot], "seq", other
            ).wait_recv()

    row = lax.broadcasted_iota(jnp.int32, (rows, rows), 0)
    column = lax.broadcasted_iota(jnp.int32, (rows, rows), 1)
    scale = math.log2(math.e) * HEAD_DIM**-0.5

    def scored(query, slot):
        pair = kv_all[slot]
        scores = lax.dot_general(
            query, pair, (((1,), (1,)), ((), ())), preferred_element_type=jnp.float32
        ) * scale
        lane = lax.broadcasted_iota(jnp.int32, pair.shape, 1)
        values = jnp.where(lane < HEAD_DIM, jnp.ones_like(pair), pair)
        return scores, values

    def absorb(state, scores, values):
        peak, total = state
        new_peak = jnp.maximum(peak, jnp.max(scores, axis=1, keepdims=True))
        weights = jnp.exp2(scores - new_peak).astype(jnp.bfloat16)
        total = total * jnp.exp2(peak - new_peak) + jnp.dot(
            weights, values, preferred_element_type=jnp.float32
        )
        return new_peak, total

    def returned(tile):
        return remote(
            ctx.at[tile], lanes(o_ref, head), ctx_send.at[tile], ctx_recv.at[head], "seq",
            chunk * heads + tile,
        )

    def near(tile, carry):
        @pl.when(tile != my_tile)
        def _():
            remote(
                q_all.at[tile], q_all.at[tile], q_send.at[0], q_recv.at[tile], "seq", other
            ).wait_recv()

        await_kv(tile + SPAN)
        query = q_all[tile]
        scores, values = scored(query, tile + SPAN)
        scores = jnp.where(column <= row, scores, -1e30)
        peak = jnp.max(scores, axis=1, keepdims=True)
        weights = jnp.exp2(scores - peak).astype(jnp.bfloat16)
        state = (peak, jnp.dot(weights, values, preferred_element_type=jnp.float32))

        def whole(back, state):
            scores, values = scored(query, tile + SPAN - back)
            return absorb(state, scores, values)

        peak, total = lax.fori_loop(1, jnp.minimum(tile, SPAN - 1) + 1, whole, state)
        peaks[tile] = peak
        totals[tile] = total
        return carry

    def far(step, carry):
        tile = heads - 1 - step
        block = chunk * heads + tile

        @pl.when(tile < SPAN)
        def _():
            await_kv(tile)

        query = q_all[tile]

        def whole(back, state):
            scores, values = scored(query, tile + SPAN - back)
            return absorb(state, scores, values)

        state = lax.fori_loop(
            jnp.minimum(tile, SPAN - 1) + 1,
            jnp.minimum(block, SPAN - 1) + 1,
            whole,
            (peaks[tile], totals[tile]),
        )

        def oldest(back, state):
            scores, values = scored(query, tile)
            return absorb(state, jnp.where(column > row, scores, -1e30), values)

        peak, total = lax.fori_loop(0, jnp.where(block >= SPAN, 1, 0), oldest, state)
        ctx[tile] = (total / total[:, :1]).astype(jnp.bfloat16)

        @pl.when(tile != my_tile)
        def _():
            returned(tile).start()

        @pl.when(tile == my_tile)
        def _():
            pltpu.make_async_copy(ctx.at[tile], lanes(o_ref, head), local.at[2]).start()

        return carry

    lax.fori_loop(0, heads, near, 0)
    for slot in range(heads, SPAN):
        await_kv(slot)
    lax.fori_loop(0, heads, far, 0)

    pltpu.make_async_copy(ctx.at[my_tile], lanes(o_ref, head), local.at[2]).wait()
    for tile in range(heads):
        @pl.when(tile != my_tile)
        def _():
            returned(tile).wait_send()
            remote(
                ctx.at[tile], lanes(o_ref, tile), ctx_send.at[tile], ctx_recv.at[tile], "seq", other
            ).wait_recv()

    for k in range(1, n):
        wanted, same, kv_copy, q_copy = outgoing(k)

        @pl.when(same)
        def _():
            q_copy.wait_send()

        @pl.when(wanted)
        def _():
            kv_copy.wait_send()


def attend(query, pairs, identity):
    n = lax.axis_size("seq")
    rows = query.shape[0]
    heads = query.shape[1] // LANES
    return pl.pallas_call(
        functools.partial(attention_kernel, n, heads),
        out_shape=jax.ShapeDtypeStruct(query.shape, jnp.bfloat16),
        in_specs=[ANY, ANY],
        out_specs=ANY,
        scratch_shapes=[
            pltpu.VMEM((heads, rows, LANES), jnp.bfloat16),
            pltpu.VMEM((SPAN + heads, rows, LANES), jnp.bfloat16),
            pltpu.VMEM((heads, rows, LANES), jnp.bfloat16),
            pltpu.VMEM((heads, rows, 1), jnp.float32),
            pltpu.VMEM((heads, rows, LANES), jnp.float32),
            pltpu.SemaphoreType.DMA((n - 1,)),
            pltpu.SemaphoreType.DMA((heads,)),
            pltpu.SemaphoreType.DMA((n - 1,)),
            pltpu.SemaphoreType.DMA((SPAN + heads,)),
            pltpu.SemaphoreType.DMA((heads,)),
            pltpu.SemaphoreType.DMA((heads,)),
            pltpu.SemaphoreType.DMA((3,)),
        ],
        compiler_params=pltpu.CompilerParams(collective_id=identity, has_side_effects=True),
    )(query, pairs)


def silu_slope(values):
    sigmoid = jax.nn.sigmoid(values)
    return sigmoid * (1.0 + values * (1.0 - sigmoid))


def contract(left, right, left_dim, right_dim):
    return lax.dot_general(
        left,
        right,
        (((left_dim,), (right_dim,)), ((), ())),
        preferred_element_type=jnp.float32,
    )


def normalize(retrieved, norm_gain):
    mean_square = jnp.mean(retrieved * retrieved, axis=-1, keepdims=True)
    return (retrieved * lax.rsqrt(mean_square + epsilon) * norm_gain).astype(jnp.bfloat16)


def narrow(x):
    return x.astype(jnp.bfloat16)


def paired(left, right):
    depth, width = right.shape
    left, right = (a.reshape(depth, width // HEAD_DIM, HEAD_DIM) for a in (left, right))
    return jnp.concatenate([left, right], axis=2).reshape(depth, 2 * width)


def shards(
    tokens,
    mem_query_w,
    mem_key_w,
    mem_value_w,
    mem_in,
    mem_out,
    forget_levels,
    momentum_levels,
    step_levels,
    plan,
    norm_gain,
    attn_query_w,
    attn_key_w,
    attn_value_w,
    attn_out_w,
):
    tok_rows, width = tokens.shape
    n_seq = lax.axis_size("seq")
    my_seq = lax.axis_index("seq")
    hidden_units = mem_out.shape[0]
    share = hidden_units // n_seq
    key_part = narrow(contract(tokens, mem_key_w, 1, 0))
    mem_key = gather(key_part, "head", 1, 0)
    mem_query = lax.all_gather(
        narrow(contract(tokens, mem_query_w, 1, 0)), "head", axis=1, tiled=True
    )
    value_part = narrow(contract(tokens, mem_value_w, 1, 0)).astype(jnp.float32)
    pair = lax.axis_size("head") <= 2
    out_narrow = narrow(mem_out)
    pre_act = contract(mem_key, narrow(mem_in), 1, 0)
    hidden = narrow(jax.nn.silu(pre_act))
    partial = contract(hidden, out_narrow, 1, 0)
    if pair:
        mine_first = lax.axis_index("head") * value_part.shape[1]
        value_wide = lax.dynamic_update_slice_in_dim(
            jnp.zeros_like(partial), value_part, mine_first, 1
        )
        residual_err = narrow(2.0 / tok_rows * whole_sum(narrow(partial - value_wide), "head", 1))
    else:
        predicted = scatter_sum(narrow(partial), "head", 1, 1)
        residual_err = gather(narrow(2.0 / tok_rows * (predicted - value_part)), "head", 1, 2)
    grad_out = contract(hidden, residual_err, 0, 0)
    slope_term = narrow(contract(residual_err, out_narrow, 1, 1) * silu_slope(pre_act))
    grad_in = contract(slope_term, mem_key, 0, 0)
    grads = narrow(jnp.concatenate([grad_in, grad_out], axis=1)).reshape(
        n_seq, share, 2 * width
    )

    def mine(array, dim):
        return lax.dynamic_slice_in_dim(array, my_seq * share, share, dim)

    first = jnp.concatenate([mine(mem_in, 1).T, mine(mem_out, 0)], axis=1)
    matches = jnp.arange(forget_levels.shape[0], dtype=jnp.int32)[:, None] == plan[0]
    chosen = [
        jnp.sum(jnp.where(matches, table, 0.0), axis=0)
        for table in (momentum_levels, forget_levels, step_levels)
    ]
    gates = jnp.pad(jnp.stack(chosen, axis=1), ((0, 0), (0, 125))).reshape(n_seq, share, 128)
    weights = evolve(grads, gates, first, 3).reshape(hidden_units, 2 * width)
    query_hidden = narrow(jax.nn.silu(contract(mem_query, weights[:, :width], 1, 1)))
    partial = narrow(contract(query_hidden, weights[:, width:], 1, 0))
    if pair:
        normed = normalize(whole_sum(partial, "head", 4), norm_gain)
    else:
        retrieved = scatter_sum(partial, "head", 0, 4)
        normed = gather(normalize(retrieved, norm_gain), "head", 0, 5)
    query_w = paired(attn_query_w, jnp.zeros_like(attn_query_w))
    pair_w = paired(attn_key_w, attn_value_w)
    att_query = narrow(contract(normed, query_w, 1, 0))
    att_pairs = narrow(contract(normed, pair_w, 1, 0))
    context = attend(att_query, att_pairs, 6)
    heads = attn_out_w.shape[0] // HEAD_DIM
    out_rows = attn_out_w.reshape(heads, HEAD_DIM, width)
    out_w = jnp.concatenate([jnp.zeros_like(out_rows), out_rows], axis=1).reshape(
        heads * LANES, width
    )
    return narrow(scatter_sum(narrow(contract(context, out_w, 1, 0)), "head", 1, 7))


def chain_kernel(
    n, layer, chunks, grads_ref, gates_ref, first_ref, query_ref, o_ref, other_ref,
    came, gates, state_in, state_out, stage, current,
    send, recv, send_gate, recv_gate, send_back, recv_back, send_z, recv_z, send_q, recv_q,
):
    me = lax.axis_index("seq")
    head = lax.axis_index("head")
    depth = me // layer
    place = lax.rem(me, layer)
    base = depth * layer
    deepest = n // layer - 1
    rows = grads_ref.shape[0] // chunks
    up = jnp.minimum(me + layer, n - 1)
    down = jnp.maximum(me - layer, 0)

    def span(j):
        return pl.ds(pl.multiple_of(j * rows, rows), rows)

    def lanes(which):
        return pl.ds(pl.multiple_of(which * LANES, LANES), LANES)

    def mate(k):
        return lax.rem(place + k, layer)

    def gate_copy(k):
        peer = mate(k)
        return remote(
            gates_ref.at[peer], gates.at[place], send_gate.at[peer], recv_gate.at[place], "seq", base + peer
        )

    def grad_copy(j, k):
        peer = mate(k)
        return remote(
            grads_ref.at[span(j), lanes(peer)], came.at[j, place], send.at[j, peer], recv.at[j, place],
            "seq", base + peer,
        )

    def back_copy(j, k):
        peer = mate(k)
        return remote(
            stage.at[j, peer], o_ref.at[span(j), lanes(place)], send_back.at[j, peer], recv_back.at[j, place],
            "seq", base + peer,
        )

    def state_copy(j):
        return remote(state_out.at[j], state_in.at[j], send_z.at[j], recv_z.at[j], "seq", up)

    query_copy = remote(query_ref, other_ref, send_q, recv_q, "head", 1 - head)

    barrier = pltpu.get_barrier_semaphore()
    for k in range(1, layer):
        pl.semaphore_signal(barrier, inc=1, device_id={"seq": base + mate(k)}, device_id_type=MESH)
    pl.semaphore_signal(barrier, inc=1, device_id={"head": 1 - head}, device_id_type=MESH)

    @pl.when(depth < deepest)
    def _():
        pl.semaphore_signal(barrier, inc=1, device_id={"seq": up}, device_id_type=MESH)

    @pl.when(depth > 0)
    def _():
        pl.semaphore_signal(barrier, inc=1, device_id={"seq": down}, device_id_type=MESH)

    pl.semaphore_wait(
        barrier, layer + jnp.where(depth < deepest, 1, 0) + jnp.where(depth > 0, 1, 0)
    )

    query_copy.start()
    for k in range(1, layer):
        gate_copy(k).start()

    def launch(j, carry):
        for k in range(1, layer):
            grad_copy(j, k).start()
        return carry

    lax.fori_loop(0, chunks, launch, 0)
    gates[place] = gates_ref[place]

    def keep(j, carry):
        came[j, place] = grads_ref[span(j), lanes(place)]
        return carry

    lax.fori_loop(0, chunks, keep, 0)
    for k in range(1, layer):
        peer = mate(k)
        remote(
            gates_ref.at[peer], gates.at[peer], send_gate.at[peer], recv_gate.at[peer], "seq", base + peer
        ).wait_recv()

    def advance(j, carry):
        for k in range(1, layer):
            peer = mate(k)
            remote(
                came.at[j, peer], came.at[j, peer], send.at[j, peer], recv.at[j, peer], "seq", base + peer
            ).wait_recv()

        @pl.when(depth > 0)
        def _():
            state_copy(j).wait_recv()
            current[0] = state_in[j, 0].astype(jnp.float32)
            current[1] = state_in[j, 1].astype(jnp.float32)

        @pl.when(depth == 0)
        def _():
            current[0] = jnp.zeros((rows, LANES), jnp.float32)
            current[1] = first_ref[span(j), :]

        speed = current[0]
        weight = current[1]
        for g in range(layer):
            stage[j, g] = weight.astype(jnp.bfloat16)
            grad = came[j, g].astype(jnp.float32)
            speed = gates[g, 0:1, :] * speed - gates[g, 2:3, :] * grad
            weight = (1.0 - gates[g, 1:2, :]) * weight + speed
        state_out[j, 0] = speed.astype(jnp.bfloat16)
        state_out[j, 1] = weight.astype(jnp.bfloat16)

        @pl.when(depth < deepest)
        def _():
            state_copy(j).start()

        for k in range(1, layer):
            back_copy(j, k).start()
        o_ref[span(j), lanes(place)] = stage[j, place]
        return carry

    lax.fori_loop(0, chunks, advance, 0)

    def finish(j, carry):
        for k in range(1, layer):
            peer = mate(k)
            grad_copy(j, k).wait_send()
            back_copy(j, k).wait_send()
            remote(
                stage.at[j, peer], o_ref.at[span(j), lanes(peer)], send_back.at[j, peer],
                recv_back.at[j, peer], "seq", base + peer,
            ).wait_recv()

        @pl.when(depth < deepest)
        def _():
            state_copy(j).wait_send()

        return carry

    lax.fori_loop(0, chunks, finish, 0)
    for k in range(1, layer):
        gate_copy(k).wait_send()
    query_copy.wait()


def chain(grads, gates, first, query, identity):
    n = lax.axis_size("seq")
    layer = gates.shape[0]
    chunks = 16
    rows = grads.shape[0] // chunks
    part_of = (chunks, layer, rows, LANES)
    return pl.pallas_call(
        functools.partial(chain_kernel, n, layer, chunks),
        out_shape=(
            jax.ShapeDtypeStruct(grads.shape, jnp.bfloat16),
            jax.ShapeDtypeStruct(query.shape, jnp.bfloat16),
        ),
        in_specs=[VMEM, VMEM, VMEM, VMEM],
        out_specs=(VMEM, VMEM),
        scratch_shapes=[
            pltpu.VMEM(part_of, jnp.bfloat16),
            pltpu.VMEM(gates.shape, jnp.float32),
            pltpu.VMEM((chunks, 2, rows, LANES), jnp.bfloat16),
            pltpu.VMEM((chunks, 2, rows, LANES), jnp.bfloat16),
            pltpu.VMEM(part_of, jnp.bfloat16),
            pltpu.VMEM((2, rows, LANES), jnp.float32),
            pltpu.SemaphoreType.DMA((chunks, layer)),
            pltpu.SemaphoreType.DMA((chunks, layer)),
            pltpu.SemaphoreType.DMA((layer,)),
            pltpu.SemaphoreType.DMA((layer,)),
            pltpu.SemaphoreType.DMA((chunks, layer)),
            pltpu.SemaphoreType.DMA((chunks, layer)),
            pltpu.SemaphoreType.DMA((chunks,)),
            pltpu.SemaphoreType.DMA((chunks,)),
            pltpu.SemaphoreType.DMA,
            pltpu.SemaphoreType.DMA,
        ],
        compiler_params=pltpu.CompilerParams(collective_id=identity, has_side_effects=True),
    )(grads, gates, first, query)


def paired_shards(
    tokens,
    mem_query_w,
    mem_key_w,
    mem_value_w,
    mem_in,
    mem_out,
    forget_levels,
    momentum_levels,
    step_levels,
    plan,
    norm_gain,
    attn_query_w,
    attn_key_w,
    attn_value_w,
    attn_out_w,
):
    tok_rows, width = tokens.shape
    my_seq = lax.axis_index("seq")
    my_head = lax.axis_index("head")
    hidden_units = mem_out.shape[0]
    layer = hidden_units // LANES
    key_part = narrow(contract(tokens, mem_key_w, 1, 0))
    mem_key = gather(key_part, "head", 1, 0)
    query_part = narrow(contract(tokens, mem_query_w, 1, 0))
    value_part = narrow(contract(tokens, mem_value_w, 1, 0)).astype(jnp.float32)
    out_narrow = narrow(mem_out)
    pre_act = contract(mem_key, narrow(mem_in), 1, 0)
    hidden = narrow(jax.nn.silu(pre_act))
    partial = contract(hidden, out_narrow, 1, 0)
    mine_first = my_head * value_part.shape[1]
    value_wide = lax.dynamic_update_slice_in_dim(
        jnp.zeros_like(partial), value_part, mine_first, 1
    )
    residual_err = narrow(2.0 / tok_rows * whole_sum(narrow(partial - value_wide), "head", 1))
    grad_out = contract(residual_err, hidden, 0, 0)
    slope_term = narrow(contract(residual_err, out_narrow, 1, 1) * silu_slope(pre_act))
    grad_in = contract(mem_key, slope_term, 0, 0)
    grads = narrow(jnp.concatenate([grad_in, grad_out], axis=0))
    place = lax.rem(my_seq, layer)

    def mine(array, dim):
        return lax.dynamic_slice_in_dim(array, place * LANES, LANES, dim)

    first = jnp.concatenate([mine(mem_in, 1), mine(mem_out, 0).T], axis=0)
    matches = jnp.arange(forget_levels.shape[0], dtype=jnp.int32)[:, None] == plan[0]
    chosen = [
        jnp.sum(jnp.where(matches, table, 0.0), axis=0)
        for table in (momentum_levels, forget_levels, step_levels)
    ]
    gates = jnp.pad(jnp.stack(chosen, axis=0), ((0, 5), (0, 0)))
    gates = gates.reshape(8, layer, LANES).transpose(1, 0, 2)
    weights, query_other = chain(grads, gates, first, query_part, 3)
    half = query_part.shape[1]
    mem_query = jnp.where(
        my_head == 0,
        jnp.concatenate([query_part, query_other], axis=1),
        jnp.concatenate([query_other, query_part], axis=1),
    )
    query_hidden = narrow(jax.nn.silu(contract(mem_query, weights[:width], 1, 0)))
    partial = narrow(contract(query_hidden, weights[width:], 1, 1))
    normed = normalize(whole_sum(partial, "head", 4), norm_gain)
    query_w = paired(attn_query_w, jnp.zeros_like(attn_query_w))
    pair_w = paired(attn_key_w, attn_value_w)
    att_query = narrow(contract(normed, query_w, 1, 0))
    att_pairs = narrow(contract(normed, pair_w, 1, 0))
    context = attend(att_query, att_pairs, 6)
    heads = attn_out_w.shape[0] // HEAD_DIM
    out_rows = attn_out_w.reshape(heads, HEAD_DIM, width)
    out_w = jnp.concatenate([jnp.zeros_like(out_rows), out_rows], axis=1).reshape(
        heads * LANES, width
    )
    return narrow(scatter_sum(narrow(contract(context, out_w, 1, 0)), "head", 1, 7))


def fits(n_seq, n_head, units):
    layer = units // n_head // LANES
    return n_head == 2 and layer * LANES * n_head == units and layer > 1 and n_seq % layer == 0


def solution(mesh):
    in_specs = (
        P("seq", None),
        P(None, "head"),
        P(None, "head"),
        P(None, "head"),
        P(None, "head"),
        P("head", None),
        P(None, "head"),
        P(None, "head"),
        P(None, "head"),
        P("seq"),
        P(),
        P(None, "head"),
        P(None, "head"),
        P(None, "head"),
        P("head", None),
    )
    out_specs = P("seq", "head")
    n_seq, n_head = mesh.shape["seq"], mesh.shape["head"]

    def block(*arrays):
        body = paired_shards if fits(n_seq, n_head, arrays[4].shape[1] * n_head) else shards
        return body(*arrays)

    return jax.shard_map(block, mesh=mesh, in_specs=in_specs, out_specs=out_specs, check_vma=False)
```

```python
import functools
import math

import jax
import jax.numpy as jnp
from jax import lax
from jax.experimental import pallas as pl
from jax.experimental.pallas import tpu as pltpu
from jax.sharding import PartitionSpec as P

HEAD_DIM = 64
LANES = 2 * HEAD_DIM
SPAN = 8
MESH = pl.DeviceIdType.MESH

epsilon = 1e-06
ANY = pl.BlockSpec(memory_space=pl.ANY)
VMEM = pl.BlockSpec(memory_space=pltpu.VMEM)


def meet(axis, n):
    me = lax.axis_index(axis)
    barrier = pltpu.get_barrier_semaphore()
    for k in range(1, n):
        pl.semaphore_signal(
            barrier, inc=1, device_id={axis: lax.rem(me + k, n)}, device_id_type=MESH
        )
    pl.semaphore_wait(barrier, n - 1)


def remote_at(src, dst, send, recv, place):
    return pltpu.make_async_remote_copy(
        src_ref=src,
        dst_ref=dst,
        send_sem=send,
        recv_sem=recv,
        device_id=place,
        device_id_type=MESH,
    )


def remote(src, dst, send, recv, axis, peer):
    return remote_at(src, dst, send, recv, {axis: peer})


def part(ref, dim, index, size):
    window = pl.ds(pl.multiple_of(index * size, size), size)
    return ref.at[:, window] if dim == 1 else ref.at[window, :]


def gather_kernel(axis, n, dim, size, x_ref, o_ref, send, recv, local):
    me = lax.axis_index(axis)
    meet(axis, n)
    slot = part(o_ref, dim, me, size)
    copies = []
    for k in range(1, n):
        copy = remote(x_ref, slot, send.at[k - 1], recv.at[k - 1], axis, lax.rem(me + k, n))
        copy.start()
        copies.append(copy)
    own = pltpu.make_async_copy(x_ref, slot, local)
    own.start()
    own.wait()
    for copy in copies:
        copy.wait()


def split_kernel(axis, n, dim, size, x_ref, o_ref, send, recv, local):
    me = lax.axis_index(axis)
    meet(axis, n)
    copies = []
    for k in range(1, n):
        peer = lax.rem(me + k, n)
        copy = remote(
            part(x_ref, dim, peer, size),
            o_ref.at[me],
            send.at[k - 1],
            recv.at[k - 1],
            axis,
            peer,
        )
        copy.start()
        copies.append(copy)
    own = pltpu.make_async_copy(part(x_ref, dim, me, size), o_ref.at[me], local)
    own.start()
    own.wait()
    for copy in copies:
        copy.wait()


def comm_call(kernel, out, n, identity, x):
    return pl.pallas_call(
        kernel,
        out_shape=out,
        in_specs=[ANY],
        out_specs=ANY,
        scratch_shapes=[
            pltpu.SemaphoreType.DMA((n - 1,)),
            pltpu.SemaphoreType.DMA((n - 1,)),
            pltpu.SemaphoreType.DMA,
        ],
        compiler_params=pltpu.CompilerParams(collective_id=identity, has_side_effects=True),
    )(x)


def gather(x, axis, dim, identity):
    n = lax.axis_size(axis)
    shape = list(x.shape)
    shape[dim] *= n
    kernel = functools.partial(gather_kernel, axis, n, dim, x.shape[dim])
    return comm_call(kernel, jax.ShapeDtypeStruct(tuple(shape), x.dtype), n, identity, x)


def scatter_sum(x, axis, dim, identity):
    n = lax.axis_size(axis)
    shape = list(x.shape)
    shape[dim] //= n
    kernel = functools.partial(split_kernel, axis, n, dim, shape[dim])
    parts = comm_call(kernel, jax.ShapeDtypeStruct((n, *shape), x.dtype), n, identity, x)
    return jnp.sum(parts.astype(jnp.float32), axis=0)


def whole_sum(x, axis, identity):
    parts = gather(x, axis, 0, identity).reshape(-1, *x.shape)
    return jnp.sum(parts.astype(jnp.float32), axis=0)


def memory_kernel(
    n, grads_ref, gates_ref, first_ref, o_ref,
    came, gates, wide, stage, send, recv, send_gate, recv_gate, send_back, recv_back, local,
):
    me = lax.axis_index("seq")
    meet("seq", n)
    copies = []
    for k in range(1, n):
        peer = lax.rem(me + k, n)
        gate_copy = remote(
            gates_ref.at[peer], gates.at[me], send_gate.at[k - 1], recv_gate.at[k - 1], "seq", peer
        )
        gate_copy.start()
        copy = remote(
            grads_ref.at[peer], came.at[me], send.at[k - 1], recv.at[k - 1], "seq", peer
        )
        copy.start()
        copies += [gate_copy, copy]
    own_gates = pltpu.make_async_copy(gates_ref.at[me], gates.at[me], local.at[0])
    own_gates.start()
    own = pltpu.make_async_copy(grads_ref.at[me], came.at[me], local.at[1])
    own.start()
    own_gates.wait()
    own.wait()
    for copy in copies:
        copy.wait()

    for g in range(n):
        row = gates[g]
        for which in range(3):
            wide[which, g] = jnp.broadcast_to(row[:, which : which + 1], row.shape)

    def columns(c, carry):
        window = pl.ds(pl.multiple_of(c * 128, 128), 128)
        weight = first_ref[:, window]
        speed = jnp.zeros_like(weight)
        for g in range(n):
            stage[g, :, window] = weight.astype(jnp.bfloat16)
            if g < n - 1:
                grad = came[g, :, window].astype(jnp.float32)
                speed = wide[0, g] * speed - wide[2, g] * grad
                weight = (1.0 - wide[1, g]) * weight + speed
        return carry

    lax.fori_loop(0, first_ref.shape[1] // 128, columns, 0)

    copies = []
    for k in range(1, n):
        peer = lax.rem(me + k, n)
        copy = remote(
            stage.at[peer], o_ref.at[me], send_back.at[k - 1], recv_back.at[k - 1], "seq", peer
        )
        copy.start()
        copies.append(copy)
    own = pltpu.make_async_copy(stage.at[me], o_ref.at[me], local.at[2])
    own.start()
    own.wait()
    for copy in copies:
        copy.wait()


def evolve(grads, gates, first, identity):
    n = grads.shape[0]
    return pl.pallas_call(
        functools.partial(memory_kernel, n),
        out_shape=jax.ShapeDtypeStruct(grads.shape, jnp.bfloat16),
        in_specs=[ANY, ANY, VMEM],
        out_specs=ANY,
        scratch_shapes=[
            pltpu.VMEM(grads.shape, jnp.bfloat16),
            pltpu.VMEM(gates.shape, jnp.float32),
            pltpu.VMEM((3, *gates.shape), jnp.float32),
            pltpu.VMEM(grads.shape, jnp.bfloat16),
            *[pltpu.SemaphoreType.DMA((n - 1,))] * 6,
            pltpu.SemaphoreType.DMA((3,)),
        ],
        compiler_params=pltpu.CompilerParams(collective_id=identity, has_side_effects=True),
    )(grads, gates, first)


def attention_kernel(
    n, heads, q_ref, kv_ref, o_ref,
    q_all, kv_all, ctx, peaks, totals, q_send, q_recv, kv_send, kv_recv, ctx_send, ctx_recv, local,
):
    me = lax.axis_index("seq")
    chunk = me // heads
    head = lax.rem(me, heads)
    other = lax.rem(me + 1, n)
    rows = q_ref.shape[0]
    slots = SPAN + heads
    first_block = chunk * heads - SPAN
    my_slot = me - first_block
    my_tile = lax.rem(me, heads)

    def lanes(ref, which):
        return ref.at[:, pl.ds(pl.multiple_of(which * LANES, LANES), LANES)]

    def outgoing(k):
        peer = lax.rem(me + k, n)
        peer_chunk = peer // heads
        peer_head = lax.rem(peer, heads)
        slot = me - peer_chunk * heads + SPAN
        wanted = jnp.logical_and(slot >= 0, slot < slots)
        same = peer_chunk == chunk
        safe = jnp.where(wanted, slot, 0)
        kv_copy = remote(
            lanes(kv_ref, peer_head), kv_all.at[safe], kv_send.at[k - 1], kv_recv.at[safe], "seq", peer
        )
        q_copy = remote(
            lanes(q_ref, peer_head), q_all.at[my_tile], q_send.at[k - 1], q_recv.at[my_tile], "seq", peer
        )
        return wanted, same, kv_copy, q_copy

    meet("seq", n)
    own_kv = pltpu.make_async_copy(lanes(kv_ref, head), kv_all.at[my_slot], local.at[0])
    own_q = pltpu.make_async_copy(lanes(q_ref, head), q_all.at[my_tile], local.at[1])
    own_kv.start()
    own_q.start()
    for k in range(1, n):
        wanted, same, kv_copy, q_copy = outgoing(k)

        @pl.when(same)
        def _():
            q_copy.start()

        @pl.when(wanted)
        def _():
            kv_copy.start()

    own_kv.wait()
    own_q.wait()

    def await_kv(slot):
        block = first_block + slot

        @pl.when(jnp.logical_and(block >= 0, block != me))
        def _():
            remote(
                kv_all.at[slot], kv_all.at[slot], kv_send.at[0], kv_recv.at[slot], "seq", other
            ).wait_recv()

    row = lax.broadcasted_iota(jnp.int32, (rows, rows), 0)
    column = lax.broadcasted_iota(jnp.int32, (rows, rows), 1)
    scale = math.log2(math.e) * HEAD_DIM**-0.5

    def scored(query, slot):
        pair = kv_all[slot]
        scores = lax.dot_general(
            query, pair, (((1,), (1,)), ((), ())), preferred_element_type=jnp.float32
        ) * scale
        lane = lax.broadcasted_iota(jnp.int32, pair.shape, 1)
        values = jnp.where(lane < HEAD_DIM, jnp.ones_like(pair), pair)
        return scores, values

    def absorb(state, scores, values):
        peak, total = state
        new_peak = jnp.maximum(peak, jnp.max(scores, axis=1, keepdims=True))
        weights = jnp.exp2(scores - new_peak).astype(jnp.bfloat16)
        total = total * jnp.exp2(peak - new_peak) + jnp.dot(
            weights, values, preferred_element_type=jnp.float32
        )
        return new_peak, total

    def returned(tile):
        return remote(
            ctx.at[tile], lanes(o_ref, head), ctx_send.at[tile], ctx_recv.at[head], "seq",
            chunk * heads + tile,
        )

    def near(tile, carry):
        @pl.when(tile != my_tile)
        def _():
            remote(
                q_all.at[tile], q_all.at[tile], q_send.at[0], q_recv.at[tile], "seq", other
            ).wait_recv()

        await_kv(tile + SPAN)
        query = q_all[tile]
        scores, values = scored(query, tile + SPAN)
        scores = jnp.where(column <= row, scores, -1e30)
        peak = jnp.max(scores, axis=1, keepdims=True)
        weights = jnp.exp2(scores - peak).astype(jnp.bfloat16)
        state = (peak, jnp.dot(weights, values, preferred_element_type=jnp.float32))

        def whole(back, state):
            scores, values = scored(query, tile + SPAN - back)
            return absorb(state, scores, values)

        peak, total = lax.fori_loop(1, jnp.minimum(tile, SPAN - 1) + 1, whole, state)
        peaks[tile] = peak
        totals[tile] = total
        return carry

    def far(step, carry):
        tile = heads - 1 - step
        block = chunk * heads + tile

        @pl.when(tile < SPAN)
        def _():
            await_kv(tile)

        query = q_all[tile]

        def whole(back, state):
            scores, values = scored(query, tile + SPAN - back)
            return absorb(state, scores, values)

        state = lax.fori_loop(
            jnp.minimum(tile, SPAN - 1) + 1,
            jnp.minimum(block, SPAN - 1) + 1,
            whole,
            (peaks[tile], totals[tile]),
        )

        def oldest(back, state):
            scores, values = scored(query, tile)
            return absorb(state, jnp.where(column > row, scores, -1e30), values)

        peak, total = lax.fori_loop(0, jnp.where(block >= SPAN, 1, 0), oldest, state)
        ctx[tile] = (total / total[:, :1]).astype(jnp.bfloat16)

        @pl.when(tile != my_tile)
        def _():
            returned(tile).start()

        @pl.when(tile == my_tile)
        def _():
            pltpu.make_async_copy(ctx.at[tile], lanes(o_ref, head), local.at[2]).start()

        return carry

    lax.fori_loop(0, heads, near, 0)
    for slot in range(heads, SPAN):
        await_kv(slot)
    lax.fori_loop(0, heads, far, 0)

    pltpu.make_async_copy(ctx.at[my_tile], lanes(o_ref, head), local.at[2]).wait()
    for tile in range(heads):
        @pl.when(tile != my_tile)
        def _():
            returned(tile).wait_send()
            remote(
                ctx.at[tile], lanes(o_ref, tile), ctx_send.at[tile], ctx_recv.at[tile], "seq", other
            ).wait_recv()

    for k in range(1, n):
        wanted, same, kv_copy, q_copy = outgoing(k)

        @pl.when(same)
        def _():
            q_copy.wait_send()

        @pl.when(wanted)
        def _():
            kv_copy.wait_send()


def attend(query, pairs, identity):
    n = lax.axis_size("seq")
    rows = query.shape[0]
    heads = query.shape[1] // LANES
    return pl.pallas_call(
        functools.partial(attention_kernel, n, heads),
        out_shape=jax.ShapeDtypeStruct(query.shape, jnp.bfloat16),
        in_specs=[ANY, ANY],
        out_specs=ANY,
        scratch_shapes=[
            pltpu.VMEM((heads, rows, LANES), jnp.bfloat16),
            pltpu.VMEM((SPAN + heads, rows, LANES), jnp.bfloat16),
            pltpu.VMEM((heads, rows, LANES), jnp.bfloat16),
            pltpu.VMEM((heads, rows, 1), jnp.float32),
            pltpu.VMEM((heads, rows, LANES), jnp.float32),
            pltpu.SemaphoreType.DMA((n - 1,)),
            pltpu.SemaphoreType.DMA((heads,)),
            pltpu.SemaphoreType.DMA((n - 1,)),
            pltpu.SemaphoreType.DMA((SPAN + heads,)),
            pltpu.SemaphoreType.DMA((heads,)),
            pltpu.SemaphoreType.DMA((heads,)),
            pltpu.SemaphoreType.DMA((3,)),
        ],
        compiler_params=pltpu.CompilerParams(collective_id=identity, has_side_effects=True),
    )(query, pairs)


def silu_slope(values):
    sigmoid = jax.nn.sigmoid(values)
    return sigmoid * (1.0 + values * (1.0 - sigmoid))


def contract(left, right, left_dim, right_dim):
    return lax.dot_general(
        left,
        right,
        (((left_dim,), (right_dim,)), ((), ())),
        preferred_element_type=jnp.float32,
    )


def normalize(retrieved, norm_gain):
    mean_square = jnp.mean(retrieved * retrieved, axis=-1, keepdims=True)
    return (retrieved * lax.rsqrt(mean_square + epsilon) * norm_gain).astype(jnp.bfloat16)


def narrow(x):
    return x.astype(jnp.bfloat16)


def paired(left, right):
    depth, width = right.shape
    left, right = (a.reshape(depth, width // HEAD_DIM, HEAD_DIM) for a in (left, right))
    return jnp.concatenate([left, right], axis=2).reshape(depth, 2 * width)


def shards(
    tokens,
    mem_query_w,
    mem_key_w,
    mem_value_w,
    mem_in,
    mem_out,
    forget_levels,
    momentum_levels,
    step_levels,
    plan,
    norm_gain,
    attn_query_w,
    attn_key_w,
    attn_value_w,
    attn_out_w,
):
    tok_rows, width = tokens.shape
    n_seq = lax.axis_size("seq")
    my_seq = lax.axis_index("seq")
    hidden_units = mem_out.shape[0]
    share = hidden_units // n_seq
    key_part = narrow(contract(tokens, mem_key_w, 1, 0))
    mem_key = gather(key_part, "head", 1, 0)
    mem_query = lax.all_gather(
        narrow(contract(tokens, mem_query_w, 1, 0)), "head", axis=1, tiled=True
    )
    value_part = narrow(contract(tokens, mem_value_w, 1, 0)).astype(jnp.float32)
    pair = lax.axis_size("head") <= 2
    out_narrow = narrow(mem_out)
    pre_act = contract(mem_key, narrow(mem_in), 1, 0)
    hidden = narrow(jax.nn.silu(pre_act))
    partial = contract(hidden, out_narrow, 1, 0)
    if pair:
        mine_first = lax.axis_index("head") * value_part.shape[1]
        value_wide = lax.dynamic_update_slice_in_dim(
            jnp.zeros_like(partial), value_part, mine_first, 1
        )
        residual_err = narrow(2.0 / tok_rows * whole_sum(narrow(partial - value_wide), "head", 1))
    else:
        predicted = scatter_sum(narrow(partial), "head", 1, 1)
        residual_err = gather(narrow(2.0 / tok_rows * (predicted - value_part)), "head", 1, 2)
    grad_out = contract(hidden, residual_err, 0, 0)
    slope_term = narrow(contract(residual_err, out_narrow, 1, 1) * silu_slope(pre_act))
    grad_in = contract(slope_term, mem_key, 0, 0)
    grads = narrow(jnp.concatenate([grad_in, grad_out], axis=1)).reshape(
        n_seq, share, 2 * width
    )

    def mine(array, dim):
        return lax.dynamic_slice_in_dim(array, my_seq * share, share, dim)

    first = jnp.concatenate([mine(mem_in, 1).T, mine(mem_out, 0)], axis=1)
    matches = jnp.arange(forget_levels.shape[0], dtype=jnp.int32)[:, None] == plan[0]
    chosen = [
        jnp.sum(jnp.where(matches, table, 0.0), axis=0)
        for table in (momentum_levels, forget_levels, step_levels)
    ]
    gates = jnp.pad(jnp.stack(chosen, axis=1), ((0, 0), (0, 125))).reshape(n_seq, share, 128)
    weights = evolve(grads, gates, first, 3).reshape(hidden_units, 2 * width)
    query_hidden = narrow(jax.nn.silu(contract(mem_query, weights[:, :width], 1, 1)))
    partial = narrow(contract(query_hidden, weights[:, width:], 1, 0))
    if pair:
        normed = normalize(whole_sum(partial, "head", 4), norm_gain)
    else:
        retrieved = scatter_sum(partial, "head", 0, 4)
        normed = gather(normalize(retrieved, norm_gain), "head", 0, 5)
    query_w = paired(attn_query_w, jnp.zeros_like(attn_query_w))
    pair_w = paired(attn_key_w, attn_value_w)
    att_query = narrow(contract(normed, query_w, 1, 0))
    att_pairs = narrow(contract(normed, pair_w, 1, 0))
    context = attend(att_query, att_pairs, 6)
    heads = attn_out_w.shape[0] // HEAD_DIM
    out_rows = attn_out_w.reshape(heads, HEAD_DIM, width)
    out_w = jnp.concatenate([jnp.zeros_like(out_rows), out_rows], axis=1).reshape(
        heads * LANES, width
    )
    return narrow(scatter_sum(narrow(contract(context, out_w, 1, 0)), "head", 1, 7))


def chain_kernel(
    n, layer, chunks, grads_ref, gates_ref, first_ref, query_ref, out_w_ref, o_ref, other_ref, far_w_ref,
    came, gates, state_in, state_out, stage, current,
    send, recv, send_gate, recv_gate, send_back, recv_back, send_z, recv_z, send_q, recv_q, send_w, recv_w,
):
    me = lax.axis_index("seq")
    head = lax.axis_index("head")
    depth = me // layer
    place = lax.rem(me, layer)
    base = depth * layer
    deepest = n // layer - 1
    rows = grads_ref.shape[0] // chunks
    up = jnp.minimum(me + layer, n - 1)
    down = jnp.maximum(me - layer, 0)

    def span(j):
        return pl.ds(pl.multiple_of(j * rows, rows), rows)

    def lanes(which):
        return pl.ds(pl.multiple_of(which * LANES, LANES), LANES)

    def mate(k):
        return lax.rem(place + k, layer)

    def gate_copy(k):
        peer = mate(k)
        return remote(
            gates_ref.at[peer], gates.at[place], send_gate.at[peer], recv_gate.at[place], "seq", base + peer
        )

    def grad_copy(j, k):
        peer = mate(k)
        return remote(
            grads_ref.at[span(j), lanes(peer)], came.at[j, place], send.at[j, peer], recv.at[j, place],
            "seq", base + peer,
        )

    def back_copy(j, k):
        peer = mate(k)
        return remote(
            stage.at[j, peer], o_ref.at[span(j), lanes(place)], send_back.at[j, peer], recv_back.at[j, place],
            "seq", base + peer,
        )

    def state_copy(j):
        return remote(state_out.at[j], state_in.at[j], send_z.at[j], recv_z.at[j], "seq", up)

    query_copy = remote(query_ref, other_ref, send_q, recv_q, "head", 1 - head)
    out_w_copy = remote(
        part(out_w_ref, 1, 1 - head, far_w_ref.shape[1]), far_w_ref, send_w, recv_w, "head", 1 - head
    )

    barrier = pltpu.get_barrier_semaphore()
    for k in range(1, layer):
        pl.semaphore_signal(barrier, inc=1, device_id={"seq": base + mate(k)}, device_id_type=MESH)
    pl.semaphore_signal(barrier, inc=1, device_id={"head": 1 - head}, device_id_type=MESH)

    @pl.when(depth < deepest)
    def _():
        pl.semaphore_signal(barrier, inc=1, device_id={"seq": up}, device_id_type=MESH)

    @pl.when(depth > 0)
    def _():
        pl.semaphore_signal(barrier, inc=1, device_id={"seq": down}, device_id_type=MESH)

    pl.semaphore_wait(
        barrier, layer + jnp.where(depth < deepest, 1, 0) + jnp.where(depth > 0, 1, 0)
    )

    query_copy.start()
    out_w_copy.start()
    for k in range(1, layer):
        gate_copy(k).start()

    def launch(j, carry):
        for k in range(1, layer):
            grad_copy(j, k).start()
        return carry

    lax.fori_loop(0, chunks, launch, 0)
    gates[place] = gates_ref[place]

    def keep(j, carry):
        came[j, place] = grads_ref[span(j), lanes(place)]
        return carry

    lax.fori_loop(0, chunks, keep, 0)
    for k in range(1, layer):
        peer = mate(k)
        remote(
            gates_ref.at[peer], gates.at[peer], send_gate.at[peer], recv_gate.at[peer], "seq", base + peer
        ).wait_recv()

    def advance(j, carry):
        for k in range(1, layer):
            peer = mate(k)
            remote(
                came.at[j, peer], came.at[j, peer], send.at[j, peer], recv.at[j, peer], "seq", base + peer
            ).wait_recv()

        @pl.when(depth > 0)
        def _():
            state_copy(j).wait_recv()
            current[0] = state_in[j, 0].astype(jnp.float32)
            current[1] = state_in[j, 1].astype(jnp.float32)

        @pl.when(depth == 0)
        def _():
            current[0] = jnp.zeros((rows, LANES), jnp.float32)
            current[1] = first_ref[span(j), :]

        speed = current[0]
        weight = current[1]
        for g in range(layer):
            stage[j, g] = weight.astype(jnp.bfloat16)
            grad = came[j, g].astype(jnp.float32)
            speed = gates[g, 0:1, :] * speed - gates[g, 2:3, :] * grad
            weight = (1.0 - gates[g, 1:2, :]) * weight + speed
        state_out[j, 0] = speed.astype(jnp.bfloat16)
        state_out[j, 1] = weight.astype(jnp.bfloat16)

        @pl.when(depth < deepest)
        def _():
            state_copy(j).start()

        for k in range(1, layer):
            back_copy(j, k).start()
        o_ref[span(j), lanes(place)] = stage[j, place]
        return carry

    lax.fori_loop(0, chunks, advance, 0)

    def finish(j, carry):
        for k in range(1, layer):
            peer = mate(k)
            grad_copy(j, k).wait_send()
            back_copy(j, k).wait_send()
            remote(
                stage.at[j, peer], o_ref.at[span(j), lanes(peer)], send_back.at[j, peer],
                recv_back.at[j, peer], "seq", base + peer,
            ).wait_recv()

        @pl.when(depth < deepest)
        def _():
            state_copy(j).wait_send()

        return carry

    lax.fori_loop(0, chunks, finish, 0)
    for k in range(1, layer):
        gate_copy(k).wait_send()
    query_copy.wait()
    out_w_copy.wait()


def chain(grads, gates, first, query, out_w, identity):
    n = lax.axis_size("seq")
    layer = gates.shape[0]
    chunks = 16
    rows = grads.shape[0] // chunks
    part_of = (chunks, layer, rows, LANES)
    return pl.pallas_call(
        functools.partial(chain_kernel, n, layer, chunks),
        out_shape=(
            jax.ShapeDtypeStruct(grads.shape, jnp.bfloat16),
            jax.ShapeDtypeStruct(query.shape, jnp.bfloat16),
            jax.ShapeDtypeStruct((out_w.shape[0], out_w.shape[1] // 2), jnp.bfloat16),
        ),
        in_specs=[VMEM] * 5,
        out_specs=(VMEM,) * 3,
        scratch_shapes=[
            pltpu.VMEM(part_of, jnp.bfloat16),
            pltpu.VMEM(gates.shape, jnp.float32),
            pltpu.VMEM((chunks, 2, rows, LANES), jnp.bfloat16),
            pltpu.VMEM((chunks, 2, rows, LANES), jnp.bfloat16),
            pltpu.VMEM(part_of, jnp.bfloat16),
            pltpu.VMEM((2, rows, LANES), jnp.float32),
            pltpu.SemaphoreType.DMA((chunks, layer)),
            pltpu.SemaphoreType.DMA((chunks, layer)),
            pltpu.SemaphoreType.DMA((layer,)),
            pltpu.SemaphoreType.DMA((layer,)),
            pltpu.SemaphoreType.DMA((chunks, layer)),
            pltpu.SemaphoreType.DMA((chunks, layer)),
            pltpu.SemaphoreType.DMA((chunks,)),
            pltpu.SemaphoreType.DMA((chunks,)),
            *[pltpu.SemaphoreType.DMA] * 4,
        ],
        compiler_params=pltpu.CompilerParams(collective_id=identity, has_side_effects=True),
    )(grads, gates, first, query, out_w)


def greet(identity_axes):
    barrier = pltpu.get_barrier_semaphore()
    for place in identity_axes:
        pl.semaphore_signal(barrier, inc=1, device_id=place, device_id_type=MESH)
    pl.semaphore_wait(barrier, len(identity_axes))


def swapped(x):
    return pltpu.roll(x, HEAD_DIM, 1)


def interleave(left, right, lane):
    first = jnp.where(lane < HEAD_DIM, left, swapped(right))
    second = jnp.where(lane < HEAD_DIM, swapped(left), right)
    return narrow(first), narrow(second)


def recall_kernel(
    chunks, own_ref, other_ref, weights_ref, gain_ref, wq_ref, wk_ref, wv_ref, q_ref, kv_ref,
    sent, came, kept, send, recv,
):
    head = lax.axis_index("head")
    rows, half = own_ref.shape
    width = 2 * half
    piece = rows // chunks // 2
    greet([{"head": 1 - head}])

    def spans(i):
        return (
            pl.ds(pl.multiple_of(i * piece, piece), piece),
            pl.ds(pl.multiple_of(rows // 2 + i * piece, piece), piece),
        )

    def exchange(i):
        return remote(sent.at[i], came.at[i], send.at[i], recv.at[i], "head", 1 - head)

    def retrieve(i, carry):
        top, bottom = spans(i)
        own = jnp.concatenate([own_ref[top, :], own_ref[bottom, :]], axis=0)
        other = jnp.concatenate([other_ref[top, :], other_ref[bottom, :]], axis=0)
        mine = weights_ref[pl.ds(pl.multiple_of(head * half, half), half), :]
        theirs = weights_ref[pl.ds(pl.multiple_of((1 - head) * half, half), half), :]
        pre_act = contract(own, mine, 1, 0) + contract(other, theirs, 1, 0)
        hidden = narrow(pre_act * jax.nn.sigmoid(pre_act))
        partial = contract(hidden, weights_ref[width:, :], 1, 1)
        kept[i] = partial
        sent[i] = narrow(partial)
        exchange(i).start()
        return carry

    lax.fori_loop(0, chunks, retrieve, 0)
    lane = lax.broadcasted_iota(jnp.int32, (piece, LANES), 1)
    tall = lax.broadcasted_iota(jnp.int32, (2 * piece, LANES), 1)

    def project_chunk(i, carry):
        exchange(i).wait_recv()
        top, bottom = spans(i)
        retrieved = kept[i] + came[i].astype(jnp.float32)
        mean_square = jnp.mean(retrieved * retrieved, axis=1, keepdims=True)
        normed = narrow(retrieved * lax.rsqrt(mean_square + epsilon) * gain_ref[...])
        query = contract(normed, wq_ref[...], 1, 0)
        keys = contract(normed, wk_ref[...], 1, 0)
        values = contract(normed, wv_ref[...], 1, 0)
        for c in range(half // LANES):
            columns = slice(c * LANES, (c + 1) * LANES)
            left = slice(2 * c * LANES, (2 * c + 1) * LANES)
            right = slice((2 * c + 1) * LANES, (2 * c + 2) * LANES)
            q_ref[top, left], q_ref[top, right] = interleave(
                query[:piece, columns], query[piece:, columns], lane
            )
            first, second = interleave(keys[:, columns], values[:, columns], tall)
            kv_ref[top, left] = first[:piece]
            kv_ref[bottom, left] = first[piece:]
            kv_ref[top, right] = second[:piece]
            kv_ref[bottom, right] = second[piece:]
        return carry

    lax.fori_loop(0, chunks, project_chunk, 0)

    def finish(i, carry):
        exchange(i).wait_send()
        return carry

    lax.fori_loop(0, chunks, finish, 0)


def recall(own, other, weights, gain, wq, wk, wv, identity):
    rows, half = own.shape
    chunks = 4
    part_of = (chunks, rows // chunks, 2 * half)
    return pl.pallas_call(
        functools.partial(recall_kernel, chunks),
        out_shape=(
            jax.ShapeDtypeStruct((rows // 2, 2 * half), jnp.bfloat16),
            jax.ShapeDtypeStruct((rows, 2 * half), jnp.bfloat16),
        ),
        in_specs=[VMEM] * 7,
        out_specs=(VMEM, VMEM),
        scratch_shapes=[
            pltpu.VMEM(part_of, jnp.bfloat16),
            pltpu.VMEM(part_of, jnp.bfloat16),
            pltpu.VMEM(part_of, jnp.float32),
            pltpu.SemaphoreType.DMA((chunks,)),
            pltpu.SemaphoreType.DMA((chunks,)),
        ],
        compiler_params=pltpu.CompilerParams(collective_id=identity, has_side_effects=True),
    )(own, other, weights, gain, wq, wk, wv)


def window_kernel(
    n, heads, split, q_ref, kv_ref, near_w_ref, far_w_ref, o_ref,
    q_all, kv_all, ctx, ctx_in, peaks, totals, w_top, w_bottom,
    q_send, q_recv, kv_send, kv_recv, ctx_send, ctx_recv,
):
    me = lax.axis_index("seq")
    plane = lax.axis_index("head")
    chunk = me // heads
    head = lax.rem(me, heads)
    other = lax.rem(me + 1, n)
    piece = q_ref.shape[0]

    def ranges(which):
        early = which == 0
        first = jnp.where(early, 0, split)
        last = jnp.where(early, split, n)
        oldest = jnp.where(early, 0, split - SPAN)
        return first, last, oldest

    q_first, q_last, kv_first = ranges(chunk)
    near_first = chunk * heads
    tiles = q_last - q_first

    def lanes(ref, which):
        return ref.at[:, pl.ds(pl.multiple_of(which * LANES, LANES), LANES)]

    def outgoing(peer):
        first, last, oldest = ranges(peer // heads)
        peer_head = lax.rem(peer, heads)
        wants_kv = jnp.logical_and(me >= oldest, me < last)
        wants_q = jnp.logical_and(me >= first, me < last)
        slot = jnp.where(wants_kv, me - oldest, 0)
        tile = jnp.where(wants_q, me - first, 0)
        kv_copy = remote(
            lanes(kv_ref, peer_head), kv_all.at[slot], kv_send.at[peer], kv_recv.at[slot], "seq", peer
        )
        q_copy = remote(
            lanes(q_ref, peer_head), q_all.at[tile], q_send.at[peer], q_recv.at[tile], "seq", peer
        )
        return wants_kv, wants_q, kv_copy, q_copy

    def peers(act):
        def near(k, carry):
            act(chunk * heads + lax.rem(head + k, heads))
            return carry

        def far(k, carry):
            act((1 - chunk) * heads + lax.rem(head + k, heads))
            return carry

        lax.fori_loop(1, heads, near, 0)
        lax.fori_loop(0, heads, far, 0)

    def start_to(peer):
        wants_kv, wants_q, kv_copy, q_copy = outgoing(peer)

        @pl.when(wants_kv)
        def _():
            kv_copy.start()

        @pl.when(wants_q)
        def _():
            q_copy.start()

    def drain_to(peer):
        wants_kv, wants_q, kv_copy, q_copy = outgoing(peer)

        @pl.when(wants_kv)
        def _():
            kv_copy.wait_send()

        @pl.when(wants_q)
        def _():
            q_copy.wait_send()

    greet(
        [{"seq": lax.rem(me + k, n), "head": plane} for k in range(1, n)]
        + [{"seq": lax.rem(me + k, n), "head": 1 - plane} for k in range(n)]
    )
    peers(start_to)

    own_columns = pl.ds(pl.multiple_of(head * LANES, LANES), LANES)
    kv_all[me - kv_first] = kv_ref[:, own_columns]

    @pl.when(jnp.logical_and(me >= q_first, me < q_last))
    def _():
        q_all[me - q_first] = q_ref[:, own_columns]

    w_top[...] = jnp.zeros_like(w_top)
    w_bottom[...] = jnp.zeros_like(w_bottom)

    def spread(h, carry):
        source = pl.ds(pl.multiple_of(h * HEAD_DIM, HEAD_DIM), HEAD_DIM)
        for ref, side in ((near_w_ref, plane), (far_w_ref, 1 - plane)):
            start = (side * heads + h) * LANES
            w_top[pl.ds(pl.multiple_of(start, HEAD_DIM), HEAD_DIM), :] = ref[source, :]
            w_bottom[pl.ds(pl.multiple_of(start + HEAD_DIM, HEAD_DIM), HEAD_DIM), :] = ref[source, :]
        return carry

    lax.fori_loop(0, heads, spread, 0)

    def await_kv(block):
        @pl.when(block != me)
        def _():
            slot = block - kv_first
            remote(
                kv_all.at[slot], kv_all.at[slot], kv_send.at[0], kv_recv.at[slot], "seq", other
            ).wait_recv()

    row = lax.broadcasted_iota(jnp.int32, (piece, 2 * piece), 0)
    column = lax.broadcasted_iota(jnp.int32, (piece, 2 * piece), 1)
    lane = lax.broadcasted_iota(jnp.int32, (piece, LANES), 1)
    scale = math.log2(math.e) * HEAD_DIM**-0.5

    def queries(tile):
        packed = q_all[tile].astype(jnp.float32)
        top = narrow(jnp.where(lane < HEAD_DIM, packed, 0.0))
        bottom = narrow(jnp.where(lane < HEAD_DIM, swapped(packed), 0.0))
        return top, bottom

    def valued(pair):
        place = lax.broadcasted_iota(jnp.int32, pair.shape, 1)
        return jnp.where(place < HEAD_DIM, jnp.ones_like(pair), pair)

    def scored(query, pair):
        return contract(query, pair, 1, 1) * scale

    def absorb(peak, total, scores, apply):
        new_peak = jnp.maximum(peak, jnp.max(scores, axis=1, keepdims=True))
        wide = jnp.concatenate([new_peak] * (2 * piece // LANES), axis=1)
        weights = narrow(jnp.exp2(scores - wide))
        return new_peak, total * jnp.exp2(peak - new_peak) + apply(weights)

    def visit(tile, first, last, state):
        query = queries(tile)

        def whole(block, state):
            pair = kv_all[block - kv_first]
            values = valued(pair)
            fresh = []
            for part_query, (peak, total) in zip(query, state):
                fresh.append(absorb(
                    peak, total, scored(part_query, pair), lambda w: contract(w, values, 1, 0)
                ))
            return tuple(fresh)

        return lax.fori_loop(first, last, whole, state)

    def saved(tile):
        return tuple((peaks[tile, i], totals[tile, i]) for i in range(2))

    def context_copy(tile, side):
        return remote_at(
            ctx.at[tile], ctx_in.at[plane * heads + head], ctx_send.at[tile, side],
            ctx_recv.at[plane * heads + head], {"seq": q_first + tile, "head": lax.rem(plane + side, 2)},
        )

    def near(tile, carry):
        block = q_first + tile

        @pl.when(block != me)
        def _():
            remote(
                q_all.at[tile], q_all.at[tile], q_send.at[0], q_recv.at[tile], "seq", other
            ).wait_recv()

        def arrive(b, carry):
            await_kv(b)
            return carry

        lax.fori_loop(jnp.where(tile == 0, near_first, block - 1), block, arrive, 0)
        empty = (jnp.full((piece, LANES), -1e30, jnp.float32), jnp.zeros((piece, LANES), jnp.float32))
        state = visit(tile, jnp.maximum(block - SPAN + 1, near_first), block, (empty, empty))
        for i, (peak, total) in enumerate(state):
            peaks[tile, i] = peak
            totals[tile, i] = total
        return carry

    def far(step, carry):
        block = q_last - 1 - step
        tile = block - q_first

        @pl.when(step == 0)
        def _():
            await_kv(block)

        @pl.when(jnp.logical_and(block >= SPAN, block - SPAN < near_first))
        def _():
            await_kv(block - SPAN)

        state = visit(tile, jnp.maximum(block - SPAN + 1, 0), near_first, saved(tile))
        query = queries(tile)
        pair = kv_all[block - kv_first]
        values = valued(pair)

        def close(states):
            top, bottom = (total / total[:, :1] for peak, total in states)
            ctx[tile] = narrow(jnp.where(lane < HEAD_DIM, swapped(top), bottom))

        @pl.when(block < SPAN)
        def _():
            states = []
            for i, (part_query, (peak, total)) in enumerate(zip(query, state)):
                seen = column <= row + i * piece
                scores = jnp.where(seen, scored(part_query, pair), -1e30)
                states.append(absorb(peak, total, scores, lambda w: contract(w, values, 1, 0)))
            close(states)

        @pl.when(block >= SPAN)
        def _():
            old_pair = kv_all[block - SPAN - kv_first]
            old_values = valued(old_pair)
            states = []
            for i, (part_query, (peak, total)) in enumerate(zip(query, state)):
                seen = column <= row + i * piece
                scores = jnp.where(seen, scored(part_query, pair), scored(part_query, old_pair))

                def apply(w):
                    none = jnp.zeros_like(w)
                    return contract(jnp.where(seen, w, none), values, 1, 0) + contract(
                        jnp.where(seen, none, w), old_values, 1, 0
                    )

                states.append(absorb(peak, total, scores, apply))
            close(states)

        context_copy(tile, 1).start()

        @pl.when(block != me)
        def _():
            context_copy(tile, 0).start()

        @pl.when(block == me)
        def _():
            ctx_in[plane * heads + head] = ctx[tile]

        return carry

    lax.fori_loop(0, tiles, near, 0)
    lax.fori_loop(0, tiles, far, 0)

    keeper = jnp.where(me < split, 0, heads)

    def gathered(h, carry):
        for side in range(2):
            slot = lax.rem(plane + side, 2) * heads + h

            def wait():
                remote(
                    ctx_in.at[slot], ctx_in.at[slot], ctx_send.at[0, 0], ctx_recv.at[slot], "seq", other
                ).wait_recv()

            if side == 0:
                pl.when(keeper + h != me)(wait)
            else:
                wait()
        return carry

    lax.fori_loop(0, heads, gathered, 0)
    for side, weights in enumerate((w_top, w_bottom)):
        total = jnp.zeros((piece, o_ref.shape[1]), jnp.float32)
        for h in range(heads):
            both = jnp.concatenate([ctx_in[2 * h], ctx_in[2 * h + 1]], axis=1)
            total += contract(both, weights[2 * h * LANES : 2 * (h + 1) * LANES, :], 1, 0)
        o_ref[side * piece : (side + 1) * piece, :] = narrow(total)

    def sent(tile, carry):
        context_copy(tile, 1).wait_send()

        @pl.when(q_first + tile != me)
        def _():
            context_copy(tile, 0).wait_send()

        return carry

    lax.fori_loop(0, tiles, sent, 0)
    peers(drain_to)


def balance(n):
    costs = [min(b, SPAN) + 1 for b in range(n)]
    return min(range(SPAN, n), key=lambda s: max(sum(costs[:s]), sum(costs[s:])))


def window(query, pairs, near_w, far_w, identity):
    n = lax.axis_size("seq")
    piece = query.shape[0]
    heads = query.shape[1] // LANES
    split = balance(n)
    tiles = max(split, n - split)
    slots = max(split, n - split + SPAN)
    wide = (2 * heads * LANES, near_w.shape[1])
    return pl.pallas_call(
        functools.partial(window_kernel, n, heads, split),
        out_shape=jax.ShapeDtypeStruct((2 * piece, near_w.shape[1]), jnp.bfloat16),
        in_specs=[VMEM] * 4,
        out_specs=VMEM,
        scratch_shapes=[
            pltpu.VMEM((tiles, piece, LANES), jnp.bfloat16),
            pltpu.VMEM((slots, 2 * piece, LANES), jnp.bfloat16),
            pltpu.VMEM((tiles, piece, LANES), jnp.bfloat16),
            pltpu.VMEM((2 * heads, piece, LANES), jnp.bfloat16),
            pltpu.VMEM((tiles, 2, piece, LANES), jnp.float32),
            pltpu.VMEM((tiles, 2, piece, LANES), jnp.float32),
            pltpu.VMEM(wide, jnp.bfloat16),
            pltpu.VMEM(wide, jnp.bfloat16),
            pltpu.SemaphoreType.DMA((n,)),
            pltpu.SemaphoreType.DMA((tiles,)),
            pltpu.SemaphoreType.DMA((n,)),
            pltpu.SemaphoreType.DMA((slots,)),
            pltpu.SemaphoreType.DMA((tiles, 2)),
            pltpu.SemaphoreType.DMA((2 * heads,)),
        ],
        compiler_params=pltpu.CompilerParams(collective_id=identity, has_side_effects=True),
    )(query, pairs, near_w, far_w)


def paired_shards(
    tokens,
    mem_query_w,
    mem_key_w,
    mem_value_w,
    mem_in,
    mem_out,
    forget_levels,
    momentum_levels,
    step_levels,
    plan,
    norm_gain,
    attn_query_w,
    attn_key_w,
    attn_value_w,
    attn_out_w,
):
    tok_rows, width = tokens.shape
    my_seq = lax.axis_index("seq")
    my_head = lax.axis_index("head")
    hidden_units = mem_out.shape[0]
    layer = hidden_units // LANES
    key_part = narrow(contract(tokens, mem_key_w, 1, 0))
    mem_key = gather(key_part, "head", 1, 0)
    query_part = narrow(contract(tokens, mem_query_w, 1, 0))
    value_part = narrow(contract(tokens, mem_value_w, 1, 0)).astype(jnp.float32)
    out_narrow = narrow(mem_out)
    pre_act = contract(mem_key, narrow(mem_in), 1, 0)
    hidden = narrow(jax.nn.silu(pre_act))
    partial = contract(hidden, out_narrow, 1, 0)
    mine_first = my_head * value_part.shape[1]
    value_wide = lax.dynamic_update_slice_in_dim(
        jnp.zeros_like(partial), value_part, mine_first, 1
    )
    residual_err = narrow(2.0 / tok_rows * whole_sum(narrow(partial - value_wide), "head", 1))
    grad_out = contract(residual_err, hidden, 0, 0)
    slope_term = narrow(contract(residual_err, out_narrow, 1, 1) * silu_slope(pre_act))
    grad_in = contract(mem_key, slope_term, 0, 0)
    grads = narrow(jnp.concatenate([grad_in, grad_out], axis=0))
    place = lax.rem(my_seq, layer)

    def mine(array, dim):
        return lax.dynamic_slice_in_dim(array, place * LANES, LANES, dim)

    first = jnp.concatenate([mine(mem_in, 1), mine(mem_out, 0).T], axis=0)
    matches = jnp.arange(forget_levels.shape[0], dtype=jnp.int32)[:, None] == plan[0]
    chosen = [
        jnp.sum(jnp.where(matches, table, 0.0), axis=0)
        for table in (momentum_levels, forget_levels, step_levels)
    ]
    gates = jnp.pad(jnp.stack(chosen, axis=0), ((0, 5), (0, 0)))
    gates = gates.reshape(8, layer, LANES).transpose(1, 0, 2)
    weights, query_other, far_w = chain(grads, gates, first, query_part, attn_out_w, 3)
    att_query, att_pairs = recall(
        query_part, query_other, weights, norm_gain[None, :], attn_query_w, attn_key_w, attn_value_w, 4
    )
    half = query_part.shape[1]
    near_w = lax.dynamic_slice_in_dim(attn_out_w, my_head * half, half, 1)
    return window(att_query, att_pairs, near_w, far_w, 6)


def fits(n_seq, n_head, units):
    layer = units // n_head // LANES
    heads = units // n_head // HEAD_DIM
    split_well = layer * LANES * n_head == units and layer > 1 and n_seq % layer == 0
    return n_head == 2 and split_well and heads == SPAN and n_seq == 2 * heads


def solution(mesh):
    in_specs = (
        P("seq", None),
        P(None, "head"),
        P(None, "head"),
        P(None, "head"),
        P(None, "head"),
        P("head", None),
        P(None, "head"),
        P(None, "head"),
        P(None, "head"),
        P("seq"),
        P(),
        P(None, "head"),
        P(None, "head"),
        P(None, "head"),
        P("head", None),
    )
    out_specs = P("seq", "head")
    n_seq, n_head = mesh.shape["seq"], mesh.shape["head"]

    def block(*arrays):
        body = paired_shards if fits(n_seq, n_head, arrays[4].shape[1] * n_head) else shards
        return body(*arrays)

    return jax.shard_map(block, mesh=mesh, in_specs=in_specs, out_specs=out_specs, check_vma=False)
```
